32 devices in a mesh: leaf: 4 (over y, x), blk: 8 (over z, core).
Axes of the slice: x: 2, y: 2, z: 4, core: 2. Of those that a mesh axis runs over, the one named last changes fastest.
Arguments:
- leaf_rhs: bfloat16 [10240, 256], P(('leaf', 'blk')), may hold values from -6 to 6
- leaf_inverse: bfloat16 [10240, 2560], P(('leaf', 'blk')), may hold values from -0.125 to 0.125
- leaf_lower: bfloat16 [4096, 2560], P(('leaf', 'blk')), may hold values from -0.125 to 0.125
- sep_rhs: bfloat16 [2, 2048, 256], P(None, ('leaf', 'blk')), may hold values from -6 to 6
- sep_inverse: bfloat16 [2048, 3072], P(('leaf', 'blk'))
- sep_lower: bfloat16 [4096, 1024], P(('leaf', 'blk'))
- slot_map: int32 [2, 32, 2], P(None, ('leaf', 'blk')), may hold values from 0 to 5, as said below
Outputs:
- leaf_solution: bfloat16 [10240, 256], P(('leaf', 'blk'))
- sep_solution: bfloat16 [2, 2048, 256], P(None, ('leaf', 'blk'))
The draws below stay inside these ranges and needn't reach their ends.
Inputs may be any that keep to these rules, and one draw needn't show every extreme that they name: For every level below the top, slot_map[h-1, q] holds two different numbers of 0 to 5; at the top level it holds 0 and 1 in some order.
All inputs are finite; a program needn't handle non-finite values.
Results may differ from the reference program's by a relative error of at most 0.015.
Values may be sent and summed in bfloat16 or wider, within the bound.
A program may use at most 128 MiB of HBM per device.

```python
import jax
import jax.numpy as jnp
from jax import lax

RHS = 256
PIV_DEV = 64
UPD_DEV = 128
LV = 2
POS = 32
SN0 = 2560
SEP_UNIT = 512
SEP_COLS = 3072
LOW_COLS = 1024
LEAF_ROWS = 10240
LOW_ROWS = 4096
SEP_ROWS = 2048
N_LEAF = 4
N_BLK = 8


def column_scale(columns_total):
    col_index = jnp.arange(columns_total, dtype=jnp.int32)
    height = jnp.zeros((columns_total,), jnp.float32)
    for step_index in range(1, LV + 1):
        height = height + (col_index >= SEP_UNIT * (2 ** step_index - 2)).astype(jnp.float32)
    return jax.lax.rsqrt(SEP_UNIT * jnp.exp2(height))


def scaled_block(key, row_count, columns_total):
    values = jax.random.normal(key, (row_count, columns_total), jnp.float32)
    return (values * column_scale(columns_total)[None, :]).astype(jnp.bfloat16)


def draw_sep_inverse(key, part):
    return scaled_block(jax.random.fold_in(key, 11), POS * PIV_DEV, SEP_COLS)


def draw_sep_lower(key, part):
    return scaled_block(jax.random.fold_in(key, 13), POS * UPD_DEV, LOW_COLS)


def draw_slot_map(key, part):
    scores = jax.random.randint(jax.random.fold_in(key, 17), (LV, POS, 6), 0, 1 << 26) * 8 + jnp.arange(6, dtype=jnp.int32)
    heights = jnp.arange(LV, dtype=jnp.int32)[:, None, None]
    blocked = (heights == LV - 1) & (jnp.arange(6, dtype=jnp.int32)[None, None, :] >= 2)
    scores = jnp.where(blocked, 1 << 30, scores)
    ordering = jnp.argsort(scores, axis=-1)
    return ordering[:, :, :2].astype(jnp.int32)


def steps_of(stream_key, dims, cuts, least, top_value):
    level = 1.0
    for dim, shards_of in cuts:
        steps = jax.random.uniform(jax.random.fold_in(jax.random.fold_in(stream_key, 6), dim), (shards_of,), jnp.float32, least / len(cuts), top_value / len(cuts))
        level = level * jnp.repeat(jnp.exp(steps), dims[dim] // shards_of).reshape((-1,) + (1,) * (len(dims) - 1 - dim))
    return level


def bell_draw(stream_key, extent, spread, most, split=(), kind=jnp.bfloat16):
    level = steps_of(stream_key, extent, split, -0.22, 0.18) if split else 1.0
    array = jax.random.normal(stream_key, extent, jnp.float32) * spread * level
    return jnp.minimum(jnp.maximum(array, -most), most).astype(kind)


def setup_inputs(seed: int = 0) -> dict:
    streams_of = jax.random.split(jax.random.key(seed), 8)
    leaf_rhs = bell_draw(streams_of[0], (LEAF_ROWS, RHS), 1.0, 6.0, ((0, 32),))
    leaf_inverse = bell_draw(streams_of[1], (LEAF_ROWS, SN0), SN0 ** -0.5, 0.125, ((0, 32),))
    leaf_lower = bell_draw(streams_of[2], (LOW_ROWS, SN0), SN0 ** -0.5, 0.125, ((0, 32),))
    sep_rhs = bell_draw(streams_of[3], (LV, SEP_ROWS, RHS), 1.0, 6.0, ((1, 32),))
    sep_inverse = draw_sep_inverse(jax.random.fold_in(streams_of[7], 71), 0)
    sep_lower = draw_sep_lower(jax.random.fold_in(streams_of[7], 71), 0)
    slot_map = draw_slot_map(jax.random.fold_in(streams_of[7], 71), 0)
    return dict(leaf_rhs=leaf_rhs, leaf_inverse=leaf_inverse, leaf_lower=leaf_lower, sep_rhs=sep_rhs, sep_inverse=sep_inverse, sep_lower=sep_lower, slot_map=slot_map)


HIGH = lax.Precision.HIGHEST


def product_f32(matrix, vectors):
    return jnp.dot(matrix.astype(jnp.float32), vectors.astype(jnp.float32), precision=HIGH)


def leaf_node(operands):
    inverse, lower_part, front_rows = operands
    solved = product_f32(inverse, front_rows).astype(jnp.bfloat16)
    return solved, -product_f32(lower_part, solved)


def node_solve(operands):
    return product_f32(operands[0], operands[1]).astype(jnp.bfloat16)


def node_reduce(operands):
    return product_f32(operands[0], operands[1])


def reference(leaf_rhs, leaf_inverse, leaf_lower, sep_rhs, sep_inverse, sep_lower, slot_map):
    leaf_front = leaf_rhs.reshape(N_LEAF, SN0, RHS)
    leaf_inv = leaf_inverse.reshape(N_LEAF, SN0, SN0)
    leaf_low = leaf_lower.reshape(N_LEAF, UPD_DEV * N_BLK, SN0)
    leaf_solution, update = lax.map(leaf_node, (leaf_inv, leaf_low, leaf_front))
    update = update.reshape(POS, 2, PIV_DEV, RHS)
    solutions = []
    for height in range(1, LV + 1):
        at_root = height == LV
        front_slots = 1 if at_root else 3
        targets = slot_map[height - 1]
        onehot = (targets[:, :, None] == jnp.arange(2 * front_slots, dtype=jnp.int32)[None, None, :]).astype(jnp.float32)
        mixed = jnp.einsum("qst,qspr->qtpr", onehot, update, precision=HIGH)
        own_part = mixed[:, :front_slots]
        sent_part = mixed[:, front_slots:]
        partner = jnp.bitwise_xor(jnp.arange(POS, dtype=jnp.int32), N_BLK * 2 ** (height - 1))
        front_rows = own_part + sent_part[partner]
        pivots = (sep_rhs[height - 1].reshape(POS, PIV_DEV, RHS).astype(jnp.float32) + front_rows[:, 0]).astype(jnp.bfloat16)
        width_now = SEP_UNIT * 2 ** height
        offset = SEP_UNIT * (2 ** height - 2)
        node_count = (POS * PIV_DEV) // width_now
        inverse = sep_inverse[:, offset:offset + width_now].reshape(node_count, width_now, width_now)
        solved = lax.map(node_solve, (inverse, pivots.reshape(node_count, width_now, RHS)))
        solutions.append(solved.reshape(POS * PIV_DEV, RHS))
        if not at_root:
            lower_part = sep_lower[:, offset:offset + width_now].reshape(node_count, 2 * width_now, width_now)
            product = lax.map(node_reduce, (lower_part, solved))
            remaining = front_rows[:, 1:].reshape(node_count, 2 * width_now, RHS)
            update = (remaining - product).reshape(POS, 2, PIV_DEV, RHS)
    return leaf_solution.reshape(N_LEAF * SN0, RHS), jnp.stack(solutions)
```

```python
import functools

import jax
import jax.numpy as jnp
from jax import lax
from jax.experimental import pallas as pl
from jax.experimental.pallas import tpu as pltpu
from jax.sharding import PartitionSpec as P

CHUNKS = 2
MESH = pl.DeviceIdType.MESH
F32 = jnp.float32
BF16 = jnp.bfloat16


def flipped(value, mask):
    bit = 0
    while 2**bit <= mask:
        if mask >> bit & 1:
            value = value + (1 - 2 * (value // 2**bit % 2)) * 2**bit
        bit += 1
    return value


class Links:
    def __init__(self, send_sems, recv_sems):
        self.send_sems, self.recv_sems = send_sems, recv_sems
        self.count = 0
        self.started = []

    def site(self):
        self.count += 1
        return self.count - 1

    def copy(self, site, source, target, device):
        return pltpu.make_async_remote_copy(
            src_ref=source,
            dst_ref=target,
            send_sem=self.send_sems.at[site],
            recv_sem=self.recv_sems.at[site],
            device_id=device,
            device_id_type=MESH,
        )

    def send(self, site, block, device, source=None):
        copy = self.copy(site, block if source is None else source, block, device)
        copy.start()

    def later(self, site, block, device, valid=None):
        self.started.append((site, block, device, valid))

    def arrived(self, site, block, device):
        self.copy(site, block, block, device).wait_recv()

    def drain(self):
        for site, block, device, valid in self.started:
            if valid is None:
                self.copy(site, block, block, device).wait_send()
            else:
                @pl.when(valid)
                def _(site=site, block=block, device=device):
                    self.copy(site, block, block, device).wait_send()


def products_of(levels, pivots):
    found = []
    for height in range(1, levels + 1):
        found.append((height, pivots))
        if height < levels:
            found.append((height, 2 * pivots))
    return found


def plan_sites(leaves, blks, levels, chunks):
    chips = blks // 2
    per_chunk = 2 * (4 * chips - 3)
    shared = 0
    for height, _ in products_of(levels, 1):
        others = 2 * 2**height - 1
        per_chunk += chips - 1 + others + 1
        shared += others
    return per_chunk * chunks + shared


def kernel(dims, *refs):
    leaves, blks, levels, chunks = dims
    (rhs_hbm, inv_hbm, low_hbm, srhs_hbm, sinv_hbm, slow_hbm, slots_hbm) = refs[:7]
    leaf_out, sep_out = refs[7:9]
    (inv, low, srhs, xbuf, ybuf, acc, upd, slots, send_sems, recv_sems, local_sems) = refs[9:20]
    rest = refs[20:]
    sent, got = rest[: 2 * levels : 2], rest[1 : 2 * levels : 2]
    groups = [rest[at : at + 4] for at in range(2 * levels, len(rest), 4)]

    leaf = lax.axis_index("leaf")
    blk = lax.axis_index("blk")
    chips = blks // 2
    chip = blk // 2
    core = blk % 2
    other = blk + 1 - 2 * core
    rows = rhs_hbm.shape[0]
    columns = rhs_hbm.shape[1]
    width = columns // chunks
    pivots = srhs_hbm.shape[1]
    links = Links(send_sems, recv_sems)

    def blk_of(some_chip):
        return some_chip * 2 + core

    loads = []
    for index in range(chunks):
        loads.append(
            pltpu.make_async_copy(
                rhs_hbm.at[:, pl.ds(index * width, width)],
                xbuf.at[index, pl.ds(pl.multiple_of(blk * rows, 16), rows)],
                local_sems.at[index],
            )
        )
    weight_loads = [
        pltpu.make_async_copy(source, target, local_sems.at[chunks + index])
        for index, (source, target) in enumerate(
            ((inv_hbm, inv), (low_hbm, low), (srhs_hbm, srhs), (slots_hbm, slots))
        )
    ]
    for load in loads + weight_loads:
        load.start()
    for vectors, _, _, _ in groups:
        vectors[...] = jnp.zeros_like(vectors)

    barrier = pltpu.get_barrier_semaphore()
    near = [(leaf, other)]
    near += [
        (flipped(leaf, mask), side) for mask in range(1, 2**levels) for side in (blk, other)
    ]
    ends = [(chip > 0, (leaf, blk - 2)), (chip < chips - 1, (leaf, blk + 2))]
    for valid, peer in ends:
        @pl.when(valid)
        def _(peer=peer):
            pl.semaphore_signal(barrier, inc=1, device_id=peer, device_id_type=MESH)
    for peer in near:
        pl.semaphore_signal(barrier, inc=1, device_id=peer, device_id_type=MESH)
    has_both = (chip + chips - 1) // chips + (2 * chips - 2 - chip) // chips
    pl.semaphore_wait(barrier, len(near) + has_both)

    def line_product(buf, weights, total, ready):
        depth = 2 * rows

        def piece(some_chip, some_core):
            return buf.at[pl.ds(pl.multiple_of((some_chip * 2 + some_core) * rows, 16), rows)]

        def chip_dot(some_chip):
            start = pl.multiple_of(some_chip * depth, 128)
            return jnp.dot(
                weights[:, pl.ds(start, depth)],
                buf[pl.ds(start, depth)],
                preferred_element_type=F32,
            )

        go_left = [links.site() for _ in range(chips - 1)]
        go_right = [links.site() for _ in range(chips - 1)]
        across = [links.site() for _ in range(2 * chips - 1)]
        left, right = (leaf, blk - 2), (leaf, blk + 2)
        mine = piece(chip, core)
        across_device = (leaf, other)

        has_left, has_right = chip > 0, chip < chips - 1

        @pl.when(has_left)
        def _():
            links.send(go_left[0], mine, left)

        @pl.when(has_right)
        def _():
            links.send(go_right[0], mine, right)

        links.send(across[0], mine, across_device)
        links.later(go_left[0], mine, left, has_left)
        links.later(go_right[0], mine, right, has_right)
        links.later(across[0], mine, across_device)
        yield
        links.arrived(across[0], piece(chip, 1 - core), across_device)
        ready()
        total[...] = chip_dot(chip)
        for step in range(chips - 1):
            yield
            from_right, from_left = chip + step + 1, chip - step - 1
            right_valid, left_valid = from_right < chips, from_left >= 0

            @pl.when(right_valid)
            def _():
                links.arrived(go_left[step], piece(from_right, core), right)
                if step + 1 < chips - 1:
                    @pl.when(has_left)
                    def _():
                        links.send(go_left[step + 1], piece(from_right, core), left)
                links.send(across[1 + step], piece(from_right, core), across_device)

            @pl.when(left_valid)
            def _():
                links.arrived(go_right[step], piece(from_left, core), left)
                if step + 1 < chips - 1:
                    @pl.when(has_right)
                    def _():
                        links.send(go_right[step + 1], piece(from_left, core), right)
                links.send(across[chips + step], piece(from_left, core), across_device)

            if step + 1 < chips - 1:
                links.later(
                    go_left[step + 1], mine, left, jnp.logical_and(right_valid, has_left)
                )
                links.later(
                    go_right[step + 1], mine, right, jnp.logical_and(left_valid, has_right)
                )
            links.later(across[1 + step], mine, across_device, right_valid)
            links.later(across[chips + step], mine, across_device, left_valid)
            yield

            @pl.when(right_valid)
            def _():
                links.arrived(across[1 + step], piece(from_right, 1 - core), across_device)

            @pl.when(left_valid)
            def _():
                links.arrived(across[chips + step], piece(from_left, 1 - core), across_device)

            first = jnp.where(right_valid, 0, 1)
            last = jnp.where(left_valid, 2, 1)

            def add(side, carry):
                total[...] += chip_dot(chip + (1 - 2 * side) * (step + 1))
                return carry

            lax.fori_loop(first, last, add, 0)

    wanted = products_of(levels, pivots)
    section = pivots * blks
    fetched, own_blocks = [], []

    def exchange_weights():
        for at, (height, height_rows) in enumerate(wanted):
            source = sinv_hbm if height_rows == pivots else slow_hbm
            span = 2**height
            weights = groups[at][1]
            offset = section * (span - 2)
            sites = {}
            for mask in range(span):
                local = flipped(leaf, mask) % span
                start = pl.multiple_of(offset + local * section, 128)
                block = source.at[:, pl.ds(start, section)]
                for side in range(2):
                    spot = weights.at[pl.ds((2 * mask + side) * height_rows, height_rows)]
                    if mask == 0 and side == 0:
                        own = pltpu.make_async_copy(
                            block, spot, local_sems.at[chunks + 4 + at]
                        )
                        own.start()
                        own_blocks.append(own)
                        continue
                    device = (flipped(leaf, mask), other if side else blk)
                    site = links.site()
                    links.send(site, spot, device, source=block)
                    links.later(site, spot, device)
                    sites[site] = (spot, device)
            fetched.append(sites)

    def weights_ready(at):
        if at in waited:
            return
        waited.add(at)
        own_blocks[at].wait()
        for site, (spot, device) in fetched[at].items():
            links.arrived(site, spot, device)

    def group_product(at, index, value):
        height, height_rows = wanted[at]
        span = 2**height
        vectors, weights, going, coming = groups[at]
        vectors = vectors.at[index]

        def piece(some_chip):
            return vectors.at[
                pl.ds(pl.multiple_of((some_chip * 2 + core) * pivots, 16), pivots)
            ]

        mine = pl.ds(pl.multiple_of(blk * pivots, 16), pivots)
        vectors[mine] = value
        along = [links.site() for _ in range(1, chips)]
        for step in range(chips - 1, 0, -1):
            device = (leaf, blk_of((chip + step) % chips))
            links.send(along[step - 1], piece(chip), device)
            links.later(along[step - 1], piece(chip), device)
        yield
        weights_ready(at)
        for step in range(1, chips):
            source = (chip + chips - step) % chips
            links.arrived(along[step - 1], piece(source), (leaf, blk_of(source)))
        parts = jnp.dot(weights[...], vectors[...], preferred_element_type=F32)
        going[index] = parts.astype(BF16)
        pending = []
        for spot in range(2 * span - 1, 0, -1):
            mask, side = spot // 2, spot % 2
            device = (flipped(leaf, mask), other if side else blk)
            block = pl.ds(spot * height_rows, height_rows)
            site = links.site()
            target = coming.at[index, block]
            links.send(site, target, device, source=going.at[index, block])
            links.later(site, target, device)
            pending.append((site, block, target, device))
        total = parts[:height_rows]
        yield
        for site, block, target, device in reversed(pending):
            links.arrived(site, target, device)
            total = total + coming[index, block].astype(F32)
        products[index] = total

    products = {}
    waited = set()

    def once(index):
        def wait():
            if (index,) not in waited:
                waited.add((index,))
                weight_loads[index].wait()

        return wait

    def chain(index):
        cols = pl.ds(index * width, width)
        own = pl.ds(pl.multiple_of(blk * rows, 16), rows)
        loads[index].wait()
        yield from line_product(xbuf.at[index], inv, acc.at[index], once(0))
        value = acc[index].astype(BF16)
        ybuf[index, own] = value
        leaf_out[:, cols] = value
        yield from line_product(ybuf.at[index], low, upd.at[index], once(1))
        upd[index] = -upd[index]
        for wait in (once(2), once(3)):
            wait()
        at = 0
        for height in range(1, levels + 1):
            at_root = height == levels
            kept = 1 if at_root else 3

            def mixed(slot):
                total = None
                for part in range(2):
                    weight = jnp.where(slots[height - 1, 0, part] == slot, 1.0, 0.0).astype(F32)
                    term = weight * upd[index, pl.ds(part * pivots, pivots)]
                    total = term if total is None else total + term
                return total

            partner = (flipped(leaf, 2 ** (height - 1)), blk)
            outgoing, incoming = sent[height - 1].at[index], got[height - 1].at[index]
            for first, last in ((0, 1), (1, kept)):
                if first == last:
                    continue
                for slot in range(first, last):
                    outgoing[pl.ds(slot * pivots, pivots)] = mixed(kept + slot).astype(BF16)
                part = pl.ds(first * pivots, (last - first) * pivots)
                site = links.site()
                links.send(site, incoming.at[part], partner, source=outgoing.at[part])
                links.later(site, incoming.at[part], partner)
                if first == 0:
                    first_site = site
                else:
                    rest_site, rest_part = site, part
            base = srhs[height - 1, :, cols].astype(F32) + mixed(0)
            yield
            head = pl.ds(0, pivots)
            links.arrived(first_site, incoming.at[head], partner)
            pivot = (base + incoming[head].astype(F32)).astype(BF16)
            yield from group_product(at, index, pivot)
            at += 1
            solved = products[index].astype(BF16)
            sep_out[height - 1, :, cols] = solved
            if not at_root:
                yield from group_product(at, index, solved)
                at += 1
                product = products[index]
                links.arrived(rest_site, incoming.at[rest_part], partner)
                keep = [mixed(slot) for slot in (1, 2)]
                for part in range(2):
                    upd[index, pl.ds(part * pivots, pivots)] = (
                        keep[part]
                        + incoming[pl.ds((1 + part) * pivots, pivots)].astype(F32)
                        - product[part * pivots : (part + 1) * pivots]
                    )

    running = [chain(index) for index in range(chunks)]
    started = False
    while running:
        alive = []
        for steps in running:
            try:
                next(steps)
                alive.append(steps)
            except StopIteration:
                pass
        running = alive
        if not started:
            started = True
            exchange_weights()
    assert links.count <= send_sems.shape[0]
    links.drain()


def hand_over(first, second, first_out, second_out, sems):
    copies = [
        pltpu.make_async_copy(first, first_out, sems.at[0]),
        pltpu.make_async_copy(second, second_out, sems.at[1]),
    ]
    for copy in copies:
        copy.start()
    for copy in copies:
        copy.wait()


def deliver(first, second):
    return pl.pallas_call(
        hand_over,
        out_shape=tuple(jax.ShapeDtypeStruct(x.shape, x.dtype) for x in (first, second)),
        in_specs=[pl.BlockSpec(memory_space=pltpu.VMEM)] * 2,
        out_specs=(pl.BlockSpec(memory_space=pltpu.HBM),) * 2,
        scratch_shapes=[pltpu.SemaphoreType.DMA((2,))],
        name="deliver",
    )(*[pltpu.with_memory_space_constraint(x, pltpu.VMEM) for x in (first, second)])


def on_device(dims, leaf_rhs, leaf_inverse, leaf_lower, sep_rhs, sep_inverse, sep_lower, slot_map):
    leaves, blks, levels, chunks = dims
    rows, columns = leaf_rhs.shape
    width = columns // chunks
    pivots = sep_rhs.shape[1]
    updates = leaf_lower.shape[0]
    slot_shape = slot_map.shape
    sites = plan_sites(leaves, blks, levels, chunks)
    wanted = products_of(levels, pivots)
    scratch = [
        pltpu.VMEM(leaf_inverse.shape, BF16),
        pltpu.VMEM(leaf_lower.shape, BF16),
        pltpu.VMEM(sep_rhs.shape, BF16),
        pltpu.VMEM((chunks, rows * blks, width), BF16),
        pltpu.VMEM((chunks, rows * blks, width), BF16),
        pltpu.VMEM((chunks, rows, width), F32),
        pltpu.VMEM((chunks, updates, width), F32),
        pltpu.SMEM(slot_shape, jnp.int32),
        pltpu.SemaphoreType.DMA((sites,)),
        pltpu.SemaphoreType.DMA((sites,)),
        pltpu.SemaphoreType.DMA((chunks + 4 + len(wanted),)),
    ]
    for height in range(1, levels + 1):
        kept = 1 if height == levels else 3
        scratch += [pltpu.VMEM((chunks, kept * pivots, width), BF16)] * 2
    section = pivots * blks
    for height, height_rows in wanted:
        members = 2 * 2**height * height_rows
        scratch += [
            pltpu.VMEM((chunks, section, width), BF16),
            pltpu.VMEM((members, section), BF16),
            pltpu.VMEM((chunks, members, width), BF16),
            pltpu.VMEM((chunks, members, width), BF16),
        ]
    results = pl.pallas_call(
        functools.partial(kernel, dims),
        out_shape=(
            pltpu.VMEM((rows, columns), BF16),
            pltpu.VMEM(sep_rhs.shape, BF16),
        ),
        in_specs=[pl.BlockSpec(memory_space=pltpu.HBM)] * 7,
        out_specs=(pl.BlockSpec(memory_space=pltpu.VMEM),) * 2,
        scratch_shapes=scratch,
        compiler_params=pltpu.CompilerParams(
            collective_id=0, has_side_effects=True, vmem_limit_bytes=60 * 2**20
        ),
        name="substitution",
    )(leaf_rhs, leaf_inverse, leaf_lower, sep_rhs, sep_inverse, sep_lower, slot_map)
    return deliver(*results)


def solution(mesh):
    leaves, blks = mesh.shape["leaf"], mesh.shape["blk"]

    def body(*args):
        dims = (leaves, blks, args[3].shape[0], CHUNKS)
        return on_device(dims, *args)

    return jax.shard_map(
        body,
        mesh=mesh,
        in_specs=(
            P(("leaf", "blk"), None),
            P(("leaf", "blk"), None),
            P(("leaf", "blk"), None),
            P(None, ("leaf", "blk"), None),
            P(("leaf", "blk"), None),
            P(("leaf", "blk"), None),
            P(None, ("leaf", "blk"), None),
        ),
        out_specs=(P(("leaf", "blk"), None), P(None, ("leaf", "blk"), None)),
        check_vma=False,
    )
```
